32 devices in a mesh: dp: 2 (over z, core), sp: 16 (over x, y).
Axes of the slice: x: 4, y: 4, z: 1, core: 2. Of those that a mesh axis runs over, the one named last changes fastest.
The devices are a block of a 4x4x8 slice.
Arguments:
- q: bfloat16 [64, 64, 112], P('dp'), parts along dimension 0
- k: bfloat16 [64, 2048, 64, 112], P('dp', 'sp'), parts along dimension 0
- v: bfloat16 [64, 2048, 64, 112], P('dp', 'sp'), parts along dimension 0
Outputs:
- q: bfloat16 [64, 64, 112], P('dp'), parts along dimension 0
There are 2 independent parts. The reference program is written for one: setup_inputs(seed, part) draws one part's arguments, and reference() takes and returns one part's arrays. A program takes and returns all parts, laid end to end along the dimension named above; each array names one.
All inputs are finite; a program needn't handle non-finite values.
Results may differ from the reference program's by a relative error of at most 0.012.
Values are sent between devices in bfloat16 or wider.
A program may use at most 768 MiB of HBM per device.

```python
import jax
import jax.numpy as jnp

BATCH = 32
CACHE = 2048
HEADS = 64
KV_HEADS = 64
HEAD = 112


def setup_inputs(seed: int = 0, part: int = 0) -> dict:
    kq, kk, kv = (jax.random.fold_in(k, part) for k in jax.random.split(jax.random.key(seed), 3))
    return {
        "q": (3 * jax.random.normal(kq, (BATCH, HEADS, HEAD), jnp.float32)).astype(jnp.bfloat16),
        "k": jax.random.normal(kk, (BATCH, CACHE, KV_HEADS, HEAD), jnp.float32).astype(jnp.bfloat16),
        "v": jax.random.normal(kv, (BATCH, CACHE, KV_HEADS, HEAD), jnp.float32).astype(jnp.bfloat16),
    }


def einsum(form, a, b):
    return jnp.einsum(form, a.astype(jnp.float32), b.astype(jnp.float32))


def reference(q, k, v):
    grouped = q.reshape(BATCH, KV_HEADS, -1, HEAD)
    scores = einsum("bgsd,bugd->bgsu", grouped, k) * HEAD**-0.5
    weights = jax.nn.softmax(scores, -1).astype(jnp.bfloat16)
    return einsum("bgsu,bugd->bgsd", weights, v).astype(jnp.bfloat16).reshape(BATCH, HEADS, HEAD)
```

```python
import functools

import jax
import jax.numpy as jnp
from jax import lax
from jax.experimental import pallas as pl
from jax.experimental.pallas import tpu as pltpu
from jax.sharding import PartitionSpec as P

ROWS = 16
LANES = 128
LAG = 2
BF16, F32 = jnp.bfloat16, jnp.float32


def iota(shape, dim):
    return lax.broadcasted_iota(jnp.int32, shape, dim)


def kernel(
    n, batch, heads, head,
    q_hbm, k_hbm, v_hbm, out_hbm,
    q_s, kbuf, vbuf, rep, rep_t, mask, qbd, probs, stats, factor, part, recv, done,
    q_sem, k_sem, v_sem, own_sem, st_send, st_recv, rs_send, rs_recv, ag_send, ag_recv,
):
    me = lax.axis_index("sp")
    seqs = n * ROWS // heads
    chunks = batch // seqs
    slots = kbuf.shape[0]
    flat = ROWS * head
    units = heads // ROWS
    scale = head**-0.5

    def fetch(src, buf, sem, b):
        slot = lax.rem(b, slots)
        return pltpu.make_async_copy(src.at[b], buf.at[slot], sem.at[slot])

    def remote(src, dst, send, rcv, peer):
        return pltpu.make_async_remote_copy(
            src_ref=src, dst_ref=dst, send_sem=send, recv_sem=rcv,
            device_id={"sp": peer}, device_id_type=pl.DeviceIdType.MESH,
        )

    get_q = pltpu.make_async_copy(q_hbm, q_s, q_sem)
    get_q.start()
    for b in range(slots):
        fetch(k_hbm, kbuf, k_sem, b).start()
    for b in range(slots):
        fetch(v_hbm, vbuf, v_sem, b).start()

    barrier = pltpu.get_barrier_semaphore()
    for hop in range(1, n):
        pl.semaphore_signal(
            barrier, inc=1, device_id={"sp": lax.rem(me + hop, n)}, device_id_type=pl.DeviceIdType.MESH
        )

    rep[...] = (lax.rem(iota(rep.shape, 1), head) == iota(rep.shape, 0)).astype(F32).astype(BF16)
    rep_t[...] = (lax.rem(iota(rep_t.shape, 0), head) == iota(rep_t.shape, 1)).astype(F32).astype(BF16)
    low = iota(mask.shape, 0) * head
    col = iota(mask.shape, 1)
    mask[...] = jnp.where((col >= low) & (col < low + head), 1.0, 0.0).astype(BF16)
    get_q.wait()
    pl.semaphore_wait(barrier, n - 1)

    def spread(c):
        rows = seqs * heads
        q = q_s[pl.ds(c * seqs, seqs)].reshape(rows, head)
        wide = jnp.dot(q, rep[...], preferred_element_type=F32).astype(BF16)
        m = mask[...]
        for r in range(rows // ROWS):
            qbd[pl.ds(r * ROWS, ROWS), :] = wide[r * ROWS : (r + 1) * ROWS] * m

    def pair_of(buf, slot, j):
        return jnp.concatenate(
            [buf[slot, pl.ds((2 * j + i) * flat, flat), :] for i in range(2)], axis=1
        )

    def scores(c, i, tile):
        b = c * seqs + i
        slot = lax.rem(b, slots)
        lane = iota((8, LANES), 1)
        for j in range(units // 2):
            lhs = qbd[pl.ds(i * heads + 2 * j * ROWS, 2 * ROWS), :]
            both = jnp.dot(lhs, pair_of(kbuf, slot, j), preferred_element_type=F32) * scale
            s = jnp.concatenate([both[:ROWS, :LANES], both[ROWS:, LANES:]], axis=0)
            high = jnp.max(s, -1, keepdims=True)
            p = jnp.exp(s - high)
            total = jnp.sum(p, -1, keepdims=True)
            probs[b, pl.ds(2 * j * ROWS, 2 * ROWS), :] = p
            for t in range(2 * ROWS // 8):
                at = i * (heads // 8) + 2 * j * ROWS // 8 + t
                tile = jnp.where(lane == at, high[8 * t : 8 * t + 8], tile)
                tile = jnp.where(lane == at + LANES // 2, total[8 * t : 8 * t + 8], tile)
        return tile

    def send_stats(c):
        for hop in range(1, n):
            here = stats.at[c, me]
            remote(here, here, st_send.at[c], st_recv.at[c], lax.rem(me + hop, n)).start()

    def join_stats(c):
        few = stats.at[c, pl.ds(0, n - 1)]
        remote(few, few, st_send.at[c], st_recv.at[c], me).wait_recv()
        high = stats[c, 0]
        for j in range(1, n):
            high = jnp.maximum(high, stats[c, j])
        total = jnp.zeros_like(high)
        for j in range(n):
            t = stats[c, j]
            total = total + pltpu.roll(t, LANES // 2, 1) * jnp.exp(t - high)
        factor[...] = jnp.exp(stats[c, me] - high) / total

    def weighted(c, i):
        b = c * seqs + i
        slot = lax.rem(b, slots)
        m = mask[...]
        f = factor[...]
        zero = jnp.zeros((ROWS, LANES), BF16)
        for j in range(units // 2):
            p = probs[b, pl.ds(2 * j * ROWS, 2 * ROWS), :]
            w = []
            for t in range(2 * ROWS // 8):
                at = i * (heads // 8) + 2 * j * ROWS // 8 + t
                w.append(p[8 * t : 8 * t + 8] * f[:, at : at + 1])
            w = jnp.concatenate(w, axis=0).astype(BF16)
            lhs = jnp.concatenate(
                [jnp.concatenate([w[:ROWS], zero], 1), jnp.concatenate([zero, w[ROWS:]], 1)], 0
            )
            seen = lax.dot_general(
                lhs, pair_of(vbuf, slot, j), (((1,), (1,)), ((), ())), preferred_element_type=F32
            ).astype(BF16)
            kept = jnp.concatenate([seen[:ROWS] * m, seen[ROWS:] * m], axis=0)
            res = jnp.dot(kept, rep_t[...], preferred_element_type=F32).astype(BF16)
            for t in range(2):
                part[c, i * units + 2 * j + t] = res[t * ROWS : (t + 1) * ROWS]

    def send_parts(c):
        for hop in range(1, n):
            peer = lax.rem(me + hop, n)
            remote(part.at[c, peer], recv.at[c, me], rs_send.at[c], rs_recv.at[c], peer).start()

    def own_out(c):
        return pltpu.make_async_copy(done.at[c], out_hbm.at[c * n + me], own_sem.at[c])

    def join_parts(c):
        few = recv.at[c, pl.ds(0, n - 1)]
        remote(few, few, rs_send.at[c], rs_recv.at[c], me).wait_recv()
        recv[c, me] = part[c, me]
        total = recv[c, 0].astype(F32)
        for j in range(1, n):
            total = total + recv[c, j].astype(F32)
        done[c] = total.astype(BF16)

    def send_result(c):
        for hop in range(1, n):
            remote(done.at[c], out_hbm.at[c * n + me], ag_send, ag_recv, lax.rem(me + hop, n)).start()
        own_out(c).start()

    def work(c, with_k, with_v):
        v = c - LAG
        if with_k:
            spread(c)
        if with_v:
            join_stats(v)
        tile = jnp.zeros((8, LANES), F32)
        for h in range(seqs // 2):
            mine = (2 * h, 2 * h + 1)
            for i in mine:
                if with_k:
                    fetch(k_hbm, kbuf, k_sem, c * seqs + i).wait()
                if with_v:
                    fetch(v_hbm, vbuf, v_sem, v * seqs + i).wait()
            for i in mine:
                if with_k:
                    tile = scores(c, i, tile)
                if with_v:
                    weighted(v, i)
            for i in mine:
                if with_k:
                    @pl.when(c * seqs + i + slots < batch)
                    def _():
                        fetch(k_hbm, kbuf, k_sem, c * seqs + i + slots).start()
                if with_v:
                    @pl.when(v * seqs + i + slots < batch)
                    def _():
                        fetch(v_hbm, vbuf, v_sem, v * seqs + i + slots).start()
        if with_k:
            stats[c, me] = tile
            send_stats(c)
        if with_v:
            send_parts(v)

            @pl.when(v >= 1)
            def _():
                join_parts(v - 1)
                send_result(v - 1)

    @pl.loop(0, LAG)
    def _(c):
        work(c, True, False)

    @pl.loop(LAG, chunks)
    def _(c):
        work(c, True, True)

    @pl.loop(chunks, chunks + LAG)
    def _(c):
        work(c, False, True)

    last = chunks - 1
    join_parts(last)
    send_result(last)
    few = out_hbm.at[pl.ds(0, chunks * (n - 1))]
    remote(few, few, ag_send, ag_recv, me).wait_recv()
    remote(few, few, ag_send, ag_recv, me).wait_send()

    @pl.loop(0, chunks)
    def _(c):
        own_out(c).wait()
        few = stats.at[c, pl.ds(0, n - 1)]
        remote(few, few, st_send.at[c], st_recv.at[c], me).wait_send()
        few = recv.at[c, pl.ds(0, n - 1)]
        remote(few, few, rs_send.at[c], rs_recv.at[c], me).wait_send()


def solution(mesh):
    n = mesh.shape["sp"]

    def step(q, k, v):
        batch, tokens, heads, head = k.shape
        flat = ROWS * head
        seqs = n * ROWS // heads
        chunks = batch // seqs
        slots = 2 * seqs
        rows_of = lambda x: x.transpose(0, 2, 3, 1).reshape(batch, heads * head, tokens)
        dma = pltpu.SemaphoreType.DMA
        out = pl.pallas_call(
            functools.partial(kernel, n, batch, heads, head),
            out_shape=jax.ShapeDtypeStruct((chunks * n, ROWS, LANES), BF16),
            in_specs=[pl.BlockSpec(memory_space=pl.ANY)] * 3,
            out_specs=pl.BlockSpec(memory_space=pl.ANY),
            scratch_shapes=[
                pltpu.VMEM((batch, heads, head), BF16),
                pltpu.VMEM((slots, heads * head, tokens), BF16),
                pltpu.VMEM((slots, heads * head, tokens), BF16),
                pltpu.VMEM((head, flat), BF16),
                pltpu.VMEM((flat, LANES), BF16),
                pltpu.VMEM((ROWS, flat), BF16),
                pltpu.VMEM((seqs * heads, flat), BF16),
                pltpu.VMEM((batch, heads, tokens), F32),
                pltpu.VMEM((chunks, n, 8, LANES), F32),
                pltpu.VMEM((8, LANES), F32),
                pltpu.VMEM((chunks, n, ROWS, LANES), BF16),
                pltpu.VMEM((chunks, n, ROWS, LANES), BF16),
                pltpu.VMEM((chunks, ROWS, LANES), BF16),
                dma, dma((slots,)), dma((slots,)), dma((chunks,)),
                dma((chunks,)), dma((chunks,)), dma((chunks,)), dma((chunks,)), dma, dma,
            ],
            compiler_params=pltpu.CompilerParams(
                collective_id=0, has_side_effects=True, vmem_limit_bytes=60 * 2**20
            ),
            cost_estimate=pl.CostEstimate(
                flops=4 * k.size, bytes_accessed=4 * k.size, transcendentals=0
            ),
        )(q, rows_of(k), rows_of(v))
        return out.reshape(batch, heads, LANES)[:, :, :head]

    return jax.shard_map(
        step,
        mesh=mesh,
        in_specs=(P("dp", None, None), P("dp", "sp", None, None), P("dp", "sp", None, None)),
        out_specs=P("dp", None, None),
        check_vma=False,
    )
```

```python
import functools

import jax
import jax.numpy as jnp
from jax import lax
from jax.experimental import pallas as pl
from jax.experimental.pallas import tpu as pltpu
from jax.sharding import PartitionSpec as P

ROWS = 16
LANES = 128
LAG = 3
JOIN = 3
BF16, F32 = jnp.bfloat16, jnp.float32


def iota(shape, dim):
    return lax.broadcasted_iota(jnp.int32, shape, dim)


def kernel(
    n, batch, heads, head,
    q_hbm, k_hbm, v_hbm, out_hbm,
    q_s, kbuf, vbuf, rep, rep_t, mask, qbd, probs, stats, factor, part, recv, done,
    q_sem, k_sem, v_sem, own_sem, st_send, st_recv, rs_send, rs_recv, ag_send, ag_recv,
):
    me = lax.axis_index("sp")
    seqs = n * ROWS // heads
    chunks = batch // seqs
    slots = kbuf.shape[0]
    flat = ROWS * head
    units = heads // ROWS
    scale = head**-0.5

    def fetch(src, buf, sem, b):
        slot = lax.rem(b, slots)
        return pltpu.make_async_copy(src.at[b], buf.at[slot], sem.at[slot])

    def remote(src, dst, send, rcv, peer):
        return pltpu.make_async_remote_copy(
            src_ref=src, dst_ref=dst, send_sem=send, recv_sem=rcv,
            device_id={"sp": peer}, device_id_type=pl.DeviceIdType.MESH,
        )

    get_q = pltpu.make_async_copy(q_hbm, q_s, q_sem)
    get_q.start()
    for b in range(slots):
        fetch(k_hbm, kbuf, k_sem, b).start()

    barrier = pltpu.get_barrier_semaphore()
    for hop in range(1, n):
        pl.semaphore_signal(
            barrier, inc=1, device_id={"sp": lax.rem(me + hop, n)}, device_id_type=pl.DeviceIdType.MESH
        )

    rep[...] = (lax.rem(iota(rep.shape, 1), head) == iota(rep.shape, 0)).astype(F32).astype(BF16)
    rep_t[...] = (lax.rem(iota(rep_t.shape, 0), head) == iota(rep_t.shape, 1)).astype(F32).astype(BF16)
    low = iota(mask.shape, 0) * head
    col = iota(mask.shape, 1)
    mask[...] = jnp.where((col >= low) & (col < low + head), 1.0, 0.0).astype(BF16)
    get_q.wait()
    pl.semaphore_wait(barrier, n - 1)

    def spread(c):
        rows = seqs * heads
        q = q_s[pl.ds(c * seqs, seqs)].reshape(rows, head)
        wide = jnp.dot(q, rep[...], preferred_element_type=F32).astype(BF16)
        m = mask[...]
        for r in range(rows // ROWS):
            qbd[pl.ds(r * ROWS, ROWS), :] = wide[r * ROWS : (r + 1) * ROWS] * m

    def pair_of(buf, slot, j):
        return jnp.concatenate(
            [buf[slot, pl.ds((2 * j + i) * flat, flat), :] for i in range(2)], axis=1
        )

    def scores(c, i, tile):
        b = c * seqs + i
        slot = lax.rem(b, slots)
        lane = iota((8, LANES), 1)
        for j in range(units // 2):
            lhs = qbd[pl.ds(i * heads + 2 * j * ROWS, 2 * ROWS), :]
            both = jnp.dot(lhs, pair_of(kbuf, slot, j), preferred_element_type=F32) * scale
            s = jnp.concatenate([both[:ROWS, :LANES], both[ROWS:, LANES:]], axis=0)
            high = jnp.max(s, -1, keepdims=True)
            p = jnp.exp(s - high)
            total = jnp.sum(p, -1, keepdims=True)
            probs[b, pl.ds(2 * j * ROWS, 2 * ROWS), :] = p
            for t in range(2 * ROWS // 8):
                at = i * (heads // 8) + 2 * j * ROWS // 8 + t
                tile = jnp.where(lane == at, high[8 * t : 8 * t + 8], tile)
                tile = jnp.where(lane == at + LANES // 2, total[8 * t : 8 * t + 8], tile)
        return tile

    def send_stats(c):
        for hop in range(1, n):
            here = stats.at[c, me]
            remote(here, here, st_send.at[c], st_recv.at[c], lax.rem(me + hop, n)).start()

    def join_stats(c):
        few = stats.at[c, pl.ds(0, n - 1)]
        remote(few, few, st_send.at[c], st_recv.at[c], me).wait_recv()
        high = stats[c, 0]
        for j in range(1, n):
            high = jnp.maximum(high, stats[c, j])
        total = jnp.zeros_like(high)
        for j in range(n):
            t = stats[c, j]
            total = total + pltpu.roll(t, LANES // 2, 1) * jnp.exp(t - high)
        factor[...] = jnp.exp(stats[c, me] - high) / total

    def weighted(c, i):
        b = c * seqs + i
        slot = lax.rem(b, slots)
        m = mask[...]
        f = factor[...]
        zero = jnp.zeros((ROWS, LANES), BF16)
        kept = []
        for j in range(units // 2):
            p = probs[b, pl.ds(2 * j * ROWS, 2 * ROWS), :]
            w = []
            for t in range(2 * ROWS // 8):
                at = i * (heads // 8) + 2 * j * ROWS // 8 + t
                w.append(p[8 * t : 8 * t + 8] * f[:, at : at + 1])
            w = jnp.concatenate(w, axis=0).astype(BF16)
            lhs = jnp.concatenate(
                [jnp.concatenate([w[:ROWS], zero], 1), jnp.concatenate([zero, w[ROWS:]], 1)], 0
            )
            seen = lax.dot_general(
                lhs, pair_of(vbuf, slot, j), (((1,), (1,)), ((), ())), preferred_element_type=F32
            ).astype(BF16)
            kept += [seen[:ROWS] * m, seen[ROWS:] * m]
        return kept

    def narrow(c, i, kept):
        res = jnp.dot(jnp.concatenate(kept, 0), rep_t[...], preferred_element_type=F32).astype(BF16)
        for t in range(len(kept)):
            part[c, i * units + t] = res[t * ROWS : (t + 1) * ROWS]

    def send_parts(c):
        for hop in range(1, n):
            peer = lax.rem(me + hop, n)
            remote(part.at[c, peer], recv.at[c, me], rs_send.at[c], rs_recv.at[c], peer).start()

    def own_out(c):
        return pltpu.make_async_copy(done.at[c], out_hbm.at[c * n + me], own_sem.at[c])

    def join_parts(c):
        few = recv.at[c, pl.ds(0, n - 1)]
        remote(few, few, rs_send.at[c], rs_recv.at[c], me).wait_recv()
        recv[c, me] = part[c, me]
        total = recv[c, 0].astype(F32)
        for j in range(1, n):
            total = total + recv[c, j].astype(F32)
        done[c] = total.astype(BF16)

    def send_result(c):
        for hop in range(1, n):
            remote(done.at[c], out_hbm.at[c * n + me], ag_send, ag_recv, lax.rem(me + hop, n)).start()
        own_out(c).start()

    def work(c, with_k, with_v):
        v = c - LAG
        if with_k:
            spread(c)
        if with_v:
            join_stats(v)
        tile = jnp.zeros((8, LANES), F32)
        for h in range(seqs // 2):
            mine = (2 * h, 2 * h + 1)
            for i in mine:
                if with_k:
                    fetch(k_hbm, kbuf, k_sem, c * seqs + i).wait()
                if with_v:
                    fetch(v_hbm, vbuf, v_sem, v * seqs + i).wait()
            kept = []
            for i in mine:
                if with_k:
                    tile = scores(c, i, tile)
                if with_v:
                    kept += weighted(v, i)
            if with_v:
                narrow(v, mine[0], kept)
            for i in mine:
                if with_k and not with_v:
                    @pl.when(c * seqs + i < slots)
                    def _():
                        fetch(v_hbm, vbuf, v_sem, c * seqs + i).start()
                if with_k:
                    @pl.when(c * seqs + i + slots < batch)
                    def _():
                        fetch(k_hbm, kbuf, k_sem, c * seqs + i + slots).start()
                if with_v:
                    @pl.when(v * seqs + i + slots < batch)
                    def _():
                        fetch(v_hbm, vbuf, v_sem, v * seqs + i + slots).start()
        if with_k:
            stats[c, me] = tile
            send_stats(c)
        if with_v:
            send_parts(v)

            @pl.when(v >= JOIN)
            def _():
                join_parts(v - JOIN)
                send_result(v - JOIN)

    @pl.loop(0, LAG)
    def _(c):
        work(c, True, False)

    @pl.loop(LAG, chunks)
    def _(c):
        work(c, True, True)

    @pl.loop(chunks, chunks + LAG)
    def _(c):
        work(c, False, True)

    @pl.loop(chunks - JOIN, chunks)
    def _(c):
        join_parts(c)
        send_result(c)

    few = out_hbm.at[pl.ds(0, chunks * (n - 1))]
    remote(few, few, ag_send, ag_recv, me).wait_recv()
    remote(few, few, ag_send, ag_recv, me).wait_send()

    @pl.loop(0, chunks)
    def _(c):
        own_out(c).wait()
        few = stats.at[c, pl.ds(0, n - 1)]
        remote(few, few, st_send.at[c], st_recv.at[c], me).wait_send()
        few = recv.at[c, pl.ds(0, n - 1)]
        remote(few, few, rs_send.at[c], rs_recv.at[c], me).wait_send()


def solution(mesh):
    n = mesh.shape["sp"]

    def step(q, k, v):
        batch, tokens, heads, head = k.shape
        flat = ROWS * head
        seqs = n * ROWS // heads
        chunks = batch // seqs
        slots = 2 * seqs
        rows_of = lambda x: x.transpose(0, 2, 3, 1).reshape(batch, heads * head, tokens)
        dma = pltpu.SemaphoreType.DMA
        out = pl.pallas_call(
            functools.partial(kernel, n, batch, heads, head),
            out_shape=jax.ShapeDtypeStruct((chunks * n, ROWS, LANES), BF16),
            in_specs=[pl.BlockSpec(memory_space=pl.ANY)] * 3,
            out_specs=pl.BlockSpec(memory_space=pl.ANY),
            scratch_shapes=[
                pltpu.VMEM((batch, heads, head), BF16),
                pltpu.VMEM((slots, heads * head, tokens), BF16),
                pltpu.VMEM((slots, heads * head, tokens), BF16),
                pltpu.VMEM((head, flat), BF16),
                pltpu.VMEM((flat, LANES), BF16),
                pltpu.VMEM((ROWS, flat), BF16),
                pltpu.VMEM((seqs * heads, flat), BF16),
                pltpu.VMEM((batch, heads, tokens), F32),
                pltpu.VMEM((chunks, n, 8, LANES), F32),
                pltpu.VMEM((8, LANES), F32),
                pltpu.VMEM((chunks, n, ROWS, LANES), BF16),
                pltpu.VMEM((chunks, n, ROWS, LANES), BF16),
                pltpu.VMEM((chunks, ROWS, LANES), BF16),
                dma, dma((slots,)), dma((slots,)), dma((chunks,)),
                dma((chunks,)), dma((chunks,)), dma((chunks,)), dma((chunks,)), dma, dma,
            ],
            compiler_params=pltpu.CompilerParams(
                collective_id=0, has_side_effects=True, vmem_limit_bytes=60 * 2**20
            ),
            cost_estimate=pl.CostEstimate(
                flops=4 * k.size, bytes_accessed=4 * k.size, transcendentals=0
            ),
        )(q, rows_of(k), rows_of(v))
        return out.reshape(batch, heads, LANES)[:, :, :head]

    return jax.shard_map(
        step,
        mesh=mesh,
        in_specs=(P("dp", None, None), P("dp", "sp", None, None), P("dp", "sp", None, None)),
        out_specs=P("dp", None, None),
        check_vma=False,
    )
```
